64 devices in a mesh: data: 4 (over x, y), expert: 16 (over z, core).
Axes of the slice: x: 2, y: 2, z: 8, core: 2. Of those that a mesh axis runs over, the one named last changes fastest.
The devices are a block of a 4x4x8 slice.
Arguments:
- x: bfloat16 [4096, 2048], P(('data', 'expert')), parts along dimension 0
- idx: int32 [4096, 6], P(('data', 'expert')), parts along dimension 0
- g: float32 [4096, 6], P(('data', 'expert')), parts along dimension 0
- hot_tok: int32 [2048], P(('data', 'expert')), parts along dimension 0
- W1: bfloat16 [64, 2048, 1408], P('expert')
- W3: bfloat16 [64, 2048, 1408], P('expert')
- W2: bfloat16 [64, 1408, 2048], P('expert')
Outputs:
- output: bfloat16 [4096, 2048], P(('data', 'expert')), parts along dimension 0
There are 4 independent parts. The reference program is written for one: setup_inputs(seed, part) draws one part's arguments, and reference() takes and returns one part's arrays. A program takes and returns all parts, laid end to end along the dimension named above; an argument that names none is the same for every part.
All inputs are finite; a program needn't handle non-finite values.
Results may differ from the reference program's by a relative error of at most 0.001.
Values are sent between devices in bfloat16 or wider.
A program may use at most 768 MiB of HBM per device.

```python
import jax
import jax.numpy as jnp
from jax import lax

EXPERTS = 64
TOP = 6
D = 2048
FF = 1408
TOKENS = 64
HOT_DIV = 2
GROUP = 16

HOT_CAP = TOKENS // HOT_DIV
COLD_CAP = 2 * ((TOKENS * TOP - HOT_CAP + EXPERTS - 2) // (EXPERTS - 1))


def _weights(key, e, fan_in, fan_out):
    keys = jax.random.split(key, e)
    return lax.map(lambda k: (jax.random.normal(k, (fan_in, fan_out), jnp.float32) * fan_in ** -0.5).astype(jnp.bfloat16), keys)


def _chip_ids(key):
    k1, k2, k3 = jax.random.split(key, 3)
    t = jnp.arange(TOKENS)[:, None]
    j = jnp.arange(TOP)[None, :]
    hot = (t < HOT_CAP) & (j == 0)
    c = jnp.where(t < HOT_CAP, t * (TOP - 1) + j - 1, HOT_CAP * (TOP - 1) + (t - HOT_CAP) * TOP + j)
    seq = jnp.concatenate([jnp.arange(EXPERTS - 1), jnp.arange((EXPERTS - 1) // 2)])
    m = EXPERTS - 1 + (EXPERTS - 1) // 2
    off = jax.random.randint(k1, (), 0, m)
    perm = jax.random.permutation(k2, EXPERTS - 1)
    ids = jnp.flip(jnp.where(hot, 0, 1 + perm[seq[(c + off) % m]]), axis=1)
    shift = jax.random.randint(k3, (), 0, TOKENS)
    ids = jnp.roll(ids, shift, axis=0)
    hot_tok = jnp.sort((jnp.arange(HOT_CAP) + shift) % TOKENS)
    return ids.astype(jnp.int32), hot_tok.astype(jnp.int32)


def setup_inputs(seed: int = 0, part: int = 0) -> dict:
    kdata, kw = jax.random.split(jax.random.PRNGKey(seed))
    kx, kr, kg = jax.random.split(jax.random.fold_in(kdata, part), 3)
    k1, k3, k2 = jax.random.split(kw, 3)
    x = jax.random.normal(kx, (GROUP * TOKENS, D), jnp.float32).astype(jnp.bfloat16)
    ids, hot = jax.vmap(_chip_ids)(jax.random.split(jax.random.fold_in(kr, 7), GROUP))
    idx = ids.reshape(GROUP * TOKENS, TOP)
    u = jax.random.uniform(kg, (GROUP * TOKENS, TOP), jnp.float32)
    g = jnp.where(idx == 0, 0.6 + 0.4 * u, 0.2 + 0.5 * u)
    return {
        'x': x,
        'idx': idx,
        'g': g,
        'hot_tok': hot.reshape(GROUP * HOT_CAP),
        'W1': _weights(k1, EXPERTS, D, FF),
        'W3': _weights(k3, EXPERTS, D, FF),
        'W2': _weights(k2, EXPERTS, FF, D),
    }


def _expert(xr, w1, w3, w2):
    a = jnp.dot(xr, w1, preferred_element_type=jnp.float32)
    b = jnp.dot(xr, w3, preferred_element_type=jnp.float32)
    u = (jax.nn.silu(a) * b).astype(jnp.bfloat16)
    return jnp.dot(u, w2, preferred_element_type=jnp.float32).astype(jnp.bfloat16)


def reference(x, idx, g, hot_tok, W1, W3, W2):
    gate = jnp.where(idx == 0, g, 0.0).sum(axis=1)
    rows = (jnp.arange(GROUP)[:, None] * TOKENS + hot_tok.reshape(GROUP, HOT_CAP)).reshape(-1)
    hh = _expert(x[rows], W1[0], W3[0], W2[0]).astype(jnp.float32)
    y = jnp.zeros((GROUP * TOKENS, D), jnp.float32).at[rows].add(gate[rows][:, None] * hh)
    flat = idx.reshape(-1)
    order = jnp.argsort(flat, stable=True)
    counts = jnp.bincount(flat, length=EXPERTS)
    starts = jnp.cumsum(counts) - counts
    cap = GROUP * COLD_CAP
    order = jnp.concatenate([order, jnp.zeros((cap,), order.dtype)])
    gflat = g.reshape(-1)

    def step(y, ew):
        e, w1, w3, w2 = ew
        r = lax.dynamic_slice(order, (starts[e],), (cap,))
        valid = jnp.arange(cap) < counts[e]
        he = _expert(x[r // TOP], w1, w3, w2).astype(jnp.float32)
        return y.at[r // TOP].add(jnp.where(valid[:, None], gflat[r][:, None] * he, 0.0)), None

    y, _ = lax.scan(step, y, (jnp.arange(1, EXPERTS), W1[1:], W3[1:], W2[1:]))
    return y.astype(jnp.bfloat16)
```

```python
import jax
import jax.numpy as jnp
from jax import lax
from jax.sharding import PartitionSpec as P


def _expert(xs, w1, w3, w2):
    a = jnp.dot(xs, w1, preferred_element_type=jnp.float32)
    b = jnp.dot(xs, w3, preferred_element_type=jnp.float32)
    u = (jax.nn.silu(a) * b).astype(jnp.bfloat16)
    return jnp.dot(u, w2, preferred_element_type=jnp.float32).astype(jnp.bfloat16)


def _split3(v):
    hi = v.astype(jnp.bfloat16)
    r = v - hi.astype(jnp.float32)
    mid = r.astype(jnp.bfloat16)
    lo = (r - mid.astype(jnp.float32)).astype(jnp.bfloat16)
    return hi, mid, lo


def solution(mesh):
    n = mesh.shape['expert']

    def local(x, idx, g, hot_tok, w1, w3, w2):
        t, d = x.shape
        k = idx.shape[1]
        el = w1.shape[0]
        e = el * n
        ch = hot_tok.shape[0]
        cap = 2 * ((t * k - ch + e - 2) // (e - 1))
        me = lax.axis_index('expert')
        xg = lax.all_gather(x, 'expert', axis=0, tiled=True)
        ig = lax.all_gather(idx, 'expert', axis=0, tiled=True)
        gg = lax.all_gather(g, 'expert', axis=0, tiled=True)
        part = jnp.zeros((n * t, d), jnp.float32)
        for l in range(el):
            rows = n * (ch if l == 0 else cap)
            hit = ig == me * el + l
            mask = hit.any(axis=1)
            gate = jnp.where(hit, gg, 0.0).sum(axis=1)
            pos = jnp.cumsum(mask.astype(jnp.int32)) - 1
            sel = (pos[None, :] == jnp.arange(rows, dtype=jnp.int32)[:, None]) & mask[None, :]
            xs = jnp.dot(sel.astype(jnp.bfloat16), xg, preferred_element_type=jnp.float32).astype(jnp.bfloat16)
            h = _expert(xs, w1[l], w3[l], w2[l])
            q = jnp.where(sel, gate[None, :], 0.0)
            for piece in _split3(q):
                part = part + lax.dot_general(piece, h, (((0,), (0,)), ((), ())), preferred_element_type=jnp.float32)
        return lax.psum_scatter(part, 'expert', scatter_dimension=0, tiled=True).astype(jnp.bfloat16)

    rows = P(('data', 'expert'))
    wspec = P('expert')
    return jax.shard_map(local, mesh=mesh, in_specs=(rows, rows, rows, rows, wspec, wspec, wspec), out_specs=rows, check_vma=False)
```

```python
import functools

import jax
import jax.numpy as jnp
from jax import lax
from jax.experimental import pallas as pl
from jax.experimental.pallas import tpu as pltpu
from jax.sharding import PartitionSpec as P

F32 = jnp.float32
BF16 = jnp.bfloat16
AG_LAGS = (1, 3, 5, 7)
AG_AHEAD = 2
AG_COMP = 8
RS_LAGS = (3, 5, 8, 11)
W13_SLOTS = 4


def _split3(v):
    hi = v.astype(BF16)
    r = v - hi.astype(F32)
    mid = r.astype(BF16)
    lo = (r - mid.astype(F32)).astype(BF16)
    return hi, mid, lo


def _kernel(cfg, x_ref, meta_ref, w1_ref, w3_ref, w2_ref, y_ref, xg, mg, w13, w2b, acc, xs, u, hc, hh, pc, ph, qc, qh, part, d2d, ring,
            x_sem, m_sem, w13_sem, w2_sem, ag_send, ag_recv, agd_recv, mg_send, mg_recv, mgd_recv, rs_send, rs_recv, rd_send, rd_recv):
    n, t, el, ch, cap, kc, nc, nk, nj = cfg
    nz = n // 2
    half = nz // 2
    ngr = n // 4
    hrow = n * ch
    crow = n * cap
    gcap = 4 * cap
    gch = 4 * ch
    gt = 4 * t
    ws = W13_SLOTS

    me = lax.axis_index('expert')
    z = me // 2
    c = me % 2
    right = ((z + 1) % nz) * 2 + c
    left = ((z + nz - 1) % nz) * 2 + c
    partner = z * 2 + (1 - c)
    nxt = (right, left)
    hot = me == 0

    def remote(src, dst, ssem, rsem, dev):
        return pltpu.make_async_remote_copy(src_ref=src, dst_ref=dst, send_sem=ssem, recv_sem=rsem, device_id={'expert': dev},
                                            device_id_type=pl.DeviceIdType.MESH)

    def base(l):
        return 0 if l == 0 else hrow + (l - 1) * crow

    def hops(k, d):
        return half - k % 2 if d == 0 else half - 1 + k % 2

    def w13_copies(k, slot):
        rows = pl.ds(k * kc, kc)
        return [pltpu.make_async_copy(w.at[l, rows, :], w13.at[slot, m, l], w13_sem.at[slot]) for m, w in enumerate((w1_ref, w3_ref)) for l in range(el)]

    def w2_copies(j, slot):
        cols = pl.ds(pl.multiple_of(j * nc, nc), nc)
        return [pltpu.make_async_copy(w2_ref.at[l, :, cols], w2b.at[slot, l], w2_sem.at[slot]) for l in range(el)]

    def x_copy(k):
        return pltpu.make_async_copy(x_ref.at[:, pl.ds(pl.multiple_of(k * kc, kc), kc)], xg.at[k, me], x_sem.at[k])

    m_copy = pltpu.make_async_copy(meta_ref, mg.at[me], m_sem)
    m_copy.start()
    for k in range(nk):
        x_copy(k).start()
    for k in range(min(ws, nk)):
        for cp in w13_copies(k, k):
            cp.start()
    for j in range(2):
        for cp in w2_copies(j, j):
            cp.start()

    barrier = pltpu.get_barrier_semaphore()
    for dev in (right, left, partner):
        pl.semaphore_signal(barrier, inc=1, device_id={'expert': dev}, device_id_type=pl.DeviceIdType.MESH)
    pl.semaphore_wait(barrier, 3)

    def own_send(k):
        x_copy(k).wait()
        blk = xg.at[k, me]
        for d in range(2):
            remote(blk, blk, ag_send, ag_recv.at[k, d, 0], nxt[d]).start()
        remote(blk, blk, ag_send, agd_recv.at[k], partner).start()

    def source(s, d):
        return ((z + (nz - s if d == 0 else s)) % nz) * 2 + c

    def ag_event(k, s, d):
        blk = xg.at[k, source(s, d)]
        remote(blk, blk, ag_send, ag_recv.at[k, d, s - 1], nxt[d]).wait_recv()

        @pl.when(s < hops(k, d))
        def _():
            remote(blk, blk, ag_send, ag_recv.at[k, d, s % half], nxt[d]).start()

        remote(blk, blk, ag_send, agd_recv.at[k], partner).start()

    def meta_event(s, d):
        blk = mg.at[source(s, d)]
        remote(blk, blk, mg_send, mg_recv.at[d, s - 1], nxt[d]).wait_recv()
        if s < half - d:
            remote(blk, blk, mg_send, mg_recv.at[d, s], nxt[d]).start()
        remote(blk, blk, mg_send, mgd_recv, partner).start()

    m_copy.wait()
    own = mg.at[me]
    for d in range(2):
        remote(own, own, mg_send, mg_recv.at[d, 0], nxt[d]).start()
    remote(own, own, mg_send, mgd_recv, partner).start()
    for k in range(AG_AHEAD):
        own_send(k)

    zb = 32

    def zero(i, carry):
        acc[0, pl.ds(pl.multiple_of(i * zb, zb), zb), :] = jnp.zeros((zb, acc.shape[2]), F32)
        acc[1, pl.ds(pl.multiple_of(i * zb, zb), zb), :] = jnp.zeros((zb, acc.shape[2]), F32)
        return carry

    lax.fori_loop(0, acc.shape[1] // zb, zero, 0)
    hc[...] = jnp.zeros(hc.shape, BF16)

    def build():
        remote(mg.at[pl.ds(0, nz)], mg.at[pl.ds(0, nz)], mg_send, mgd_recv, partner).wait_recv()
        lane1 = lax.broadcasted_iota(jnp.int32, (8, 2 * t), 1)
        s_i = lax.broadcasted_iota(jnp.int32, (gt, gt), 0)
        t_i = lax.broadcasted_iota(jnp.int32, (gt, gt), 1)
        upper = jnp.where((s_i < t_i) & (s_i // t == t_i // t), 1.0, 0.0).astype(BF16)
        blk = (lax.broadcasted_iota(jnp.int32, (1, gt), 1) // t).astype(F32)
        row_c = lax.broadcasted_iota(jnp.int32, (gcap, gt), 0).astype(F32)
        row_h = lax.broadcasted_iota(jnp.int32, (gch, gt), 0).astype(F32)
        col_c = lax.broadcasted_iota(jnp.int32, (gt, el * gcap), 1).astype(F32)
        col_h = lax.broadcasted_iota(jnp.int32, (gt, gch), 1).astype(F32)
        for g in range(ngr):
            ids, gs = [], []
            for q in range(2):
                a = mg[4 * g + 2 * q]
                b = mg[4 * g + 2 * q + 1]
                ids.append(jnp.where(lane1 < t, a, pltpu.roll(b, t, 1)))
                gs.append(jnp.where(lane1 < t, pltpu.roll(a, t, 1), b))
            ids = jnp.concatenate(ids, axis=1)
            gs = jnp.concatenate(gs, axis=1)
            masks, gates = [], []
            for l in range(el):
                e = (me * el + l).astype(F32)
                hit = ids == e
                masks.append(jnp.max(jnp.where(hit, 1.0, 0.0), axis=0, keepdims=True))
                gates.append(jnp.sum(jnp.where(hit, gs, 0.0), axis=0, keepdims=True))
            m = jnp.concatenate(masks + [jnp.zeros((16 - el, gt), F32)], axis=0)
            rank = jnp.dot(m.astype(BF16), upper, preferred_element_type=F32)
            far = jnp.full((1, gt), -4096.0, F32)
            codes = [jnp.where(masks[l] > 0.0, blk * cap + rank[l:l + 1, :], far) for l in range(el)]
            code_h = jnp.where(masks[0] > 0.0, blk * ch + rank[0:1, :], far)
            codes[0] = jnp.where(hot, far, codes[0])
            code_h = jnp.where(hot, code_h, far)
            for l in range(el):
                pc[g, l * gcap:(l + 1) * gcap, :] = jnp.where(row_c == codes[l], 1.0, 0.0).astype(BF16)
            ph[g] = jnp.where(row_h == code_h, 1.0, 0.0).astype(BF16)
            cols = jnp.concatenate(codes + gates + [code_h, jnp.zeros((16 - 2 * el - 1, gt), F32)], axis=0)
            cols = jnp.concatenate([cols, jnp.zeros((128 - 16, gt), F32)], axis=0).T
            q = jnp.zeros((gt, el * gcap), F32)
            for l in range(el):
                q = q + jnp.where(col_c == cols[:, l:l + 1] + float(l * gcap), cols[:, el + l:el + l + 1], 0.0)
            for p, piece in enumerate(_split3(q)):
                qc[g, p] = piece
            q = jnp.where(col_h == cols[:, 2 * el:2 * el + 1], cols[:, el:el + 1], 0.0)
            for p, piece in enumerate(_split3(q)):
                qh[g, p] = piece

    def k_compute(k, slot, is_hot):
        for g in range(ngr):
            xt = xg[k, 4 * g:4 * g + 4].reshape(gt, kc)
            res = jnp.dot(pc[g], xt, preferred_element_type=F32).astype(BF16)
            for l in range(1 if is_hot else 0, el):
                xs[base(l) + g * gcap:base(l) + (g + 1) * gcap, :] = res[l * gcap:(l + 1) * gcap]
            if is_hot:
                xs[g * gch:(g + 1) * gch, :] = jnp.dot(ph[g], xt, preferred_element_type=F32).astype(BF16)
        for l in range(el):
            rows = slice(base(l), base(l) + (hrow if is_hot and l == 0 else crow))
            for m in range(2):
                acc[m, rows, :] += jnp.dot(xs[rows, :], w13[slot, m, l], preferred_element_type=F32)

    def ag_round(r, carry):
        @pl.when(r + AG_AHEAD < nk)
        def _():
            own_send(r + AG_AHEAD)

        for s in range(1, half + 1):
            @pl.when(r == s)
            def _():
                for d in range(2):
                    if s <= half - d:
                        meta_event(s, d)

        def events(s):
            k = r - AG_LAGS[s - 1]
            for d in range(2):
                @pl.when((k >= 0) & (k < nk) & (s <= hops(k, d)))
                def _():
                    ag_event(k, s, d)

        for s in range(1, half):
            events(s)

        @pl.when(r == half + 2)
        def _():
            build()

        k = r - AG_COMP

        @pl.when(k >= 0)
        def _():
            slot = k % ws
            remote(xg.at[k, pl.ds(0, nz)], xg.at[k, pl.ds(0, nz)], ag_send, agd_recv.at[k], partner).wait_recv()
            for cp in w13_copies(k, slot):
                cp.wait()

            @pl.when(hot)
            def _():
                k_compute(k, slot, True)

            @pl.when(jnp.logical_not(hot))
            def _():
                k_compute(k, slot, False)

            @pl.when(k + ws < nk)
            def _():
                for cp in w13_copies(k + ws, slot):
                    cp.start()

        events(half)
        return carry

    lax.fori_loop(0, nk + AG_COMP, ag_round, 0)

    ub = 32

    def act(i, carry):
        r = i * ub
        r = pl.multiple_of(jnp.where(hot | (r < crow), r, r - crow + hrow), ub)
        rows = pl.ds(r, ub)
        u[rows, :] = (jax.nn.silu(acc[0, rows, :]) * acc[1, rows, :]).astype(BF16)
        return carry

    @pl.when(hot)
    def _():
        lax.fori_loop(0, (hrow + (el - 1) * crow) // ub, act, 0)

    @pl.when(jnp.logical_not(hot))
    def _():
        lax.fori_loop(0, (el * crow) // ub, act, 0)

    def n_compute(j, slot, buf, is_hot):
        for l in range(el):
            big = is_hot and l == 0
            rows = slice(base(l), base(l) + (hrow if big else crow))
            h = jnp.dot(u[rows, :], w2b[slot, l], preferred_element_type=F32).astype(BF16)
            for g in range(ngr):
                if big:
                    hh[g] = h[g * gch:(g + 1) * gch]
                else:
                    hc[g, l * gcap:(l + 1) * gcap, :] = h[g * gcap:(g + 1) * gcap]
        for g in range(ngr):
            tot = jnp.dot(qc[g, 0], hc[g], preferred_element_type=F32)
            for p in range(1, 3):
                tot += jnp.dot(qc[g, p], hc[g], preferred_element_type=F32)
            if is_hot:
                for p in range(3):
                    tot += jnp.dot(qh[g, p], hh[g], preferred_element_type=F32)
            part[buf, 2 * g:2 * g + 2] = tot.reshape(2, 2, t, nc)

    def d2d_copy(j, buf):
        return remote(part.at[buf, :, 1 - c], d2d.at[j], rd_send.at[buf], rd_recv.at[j], partner)

    def slot_of(s, d):
        return s - 1 if d == 0 else nz - 1 - s

    def rs_start(j):
        buf = j % 2
        d2d_copy(j, buf).wait_recv()
        for d in range(nz):
            d2d[j, d] += part[buf, d, c]
        for d in range(2):
            h = hops(j, d)
            dest = (z + h) % nz if d == 0 else (z + nz - h) % nz
            remote(d2d.at[j, dest], ring.at[j, slot_of(1, d)], rs_send, rs_recv.at[j, d, 0], nxt[d]).start()

    def rs_event(j, s, d):
        h = hops(j, d)
        dest = (z + h - s) % nz if d == 0 else (z + nz - h + s) % nz
        at = slot_of(s, d)
        here = ring.at[j, at]
        remote(here, here, rs_send, rs_recv.at[j, d, s - 1], nxt[d]).wait_recv()

        @pl.when(s < h)
        def _():
            ring[j, at] += d2d[j, dest]
            remote(here, ring.at[j, slot_of(s % half + 1, d)], rs_send, rs_recv.at[j, d, s % half], nxt[d]).start()

        @pl.when(s == h)
        def _():
            d2d[j, z] += ring[j, at]

    def rs_round(r, carry):
        @pl.when(r < nj)
        def _():
            slot = r % 2
            for cp in w2_copies(r, slot):
                cp.wait()

            @pl.when(r >= 2)
            def _():
                d2d_copy(r - 2, slot).wait_send()

            @pl.when(hot)
            def _():
                n_compute(r, slot, slot, True)

            @pl.when(jnp.logical_not(hot))
            def _():
                n_compute(r, slot, slot, False)

            d2d_copy(r, slot).start()

            @pl.when(r + 2 < nj)
            def _():
                for cp in w2_copies(r + 2, slot):
                    cp.start()

        @pl.when((r >= 1) & (r - 1 < nj))
        def _():
            rs_start(r - 1)

        for s in range(1, half + 1):
            j = r - RS_LAGS[s - 1]
            for d in range(2):
                @pl.when((j >= 0) & (j < nj) & (s <= hops(j, d)))
                def _():
                    rs_event(j, s, d)

        j = r - RS_LAGS[half - 1]

        @pl.when((j >= 0) & (j < nj))
        def _():
            y_ref[:, pl.ds(pl.multiple_of(j * nc, nc), nc)] = d2d[j, z].astype(BF16)

        return carry

    lax.fori_loop(0, nj + RS_LAGS[half - 1], rs_round, 0)

    for j in range(max(nj - 2, 0), nj):
        d2d_copy(j, j % 2).wait_send()
    remote(mg.at[pl.ds(0, n - 1)], mg.at[pl.ds(0, n - 1)], mg_send, mgd_recv, partner).wait_send()
    for k in range(nk):
        blk = xg.at[k, pl.ds(0, n - 1)]
        remote(blk, blk, ag_send, agd_recv.at[k], partner).wait_send()
    for j in range(nj):
        blk = ring.at[j]
        remote(blk, blk, rs_send, rs_recv.at[j, 0, 0], partner).wait_send()


def solution(mesh):
    n = mesh.shape['expert']

    def local(x, idx, g, hot_tok, w1, w3, w2):
        t, d = x.shape
        k = idx.shape[1]
        el, _, ff = w1.shape
        e = el * n
        ch = hot_tok.shape[0]
        cap = 2 * ((t * k - ch + e - 2) // (e - 1))
        kc = nc = 256
        nk, nj = d // kc, d // nc
        nz, ngr = n // 2, n // 4
        rows = n * ch + (el - 1) * n * cap
        ids = jnp.pad(idx.T.astype(F32), ((0, 8 - k), (0, 0)), constant_values=-1.0)
        meta = jnp.concatenate([ids, jnp.pad(g.T, ((0, 8 - k), (0, 0)))], axis=1)
        cfg = (n, t, el, ch, cap, kc, nc, nk, nj)
        dma = pltpu.SemaphoreType.DMA
        return pl.pallas_call(
            functools.partial(_kernel, cfg),
            name='moe',
            out_shape=jax.ShapeDtypeStruct((t, d), BF16),
            in_specs=[pl.BlockSpec(memory_space=pl.ANY)] * 5,
            out_specs=pl.BlockSpec(memory_space=pltpu.VMEM),
            scratch_shapes=[
                pltpu.VMEM((nk, n, t, kc), BF16),
                pltpu.VMEM((n, 8, 2 * t), F32),
                pltpu.VMEM((W13_SLOTS, 2, el, kc, ff), BF16),
                pltpu.VMEM((2, el, ff, nc), BF16),
                pltpu.VMEM((2, rows, ff), F32),
                pltpu.VMEM((rows, kc), BF16),
                pltpu.VMEM((rows, ff), BF16),
                pltpu.VMEM((ngr, el * 4 * cap, nc), BF16),
                pltpu.VMEM((ngr, 4 * ch, nc), BF16),
                pltpu.VMEM((ngr, el * 4 * cap, 4 * t), BF16),
                pltpu.VMEM((ngr, 4 * ch, 4 * t), BF16),
                pltpu.VMEM((ngr, 3, 4 * t, el * 4 * cap), BF16),
                pltpu.VMEM((ngr, 3, 4 * t, 4 * ch), BF16),
                pltpu.VMEM((2, nz, 2, t, nc), F32),
                pltpu.VMEM((nj, nz, t, nc), F32),
                pltpu.VMEM((nj, nz - 1, t, nc), F32),
                dma((nk,)), dma(()), dma((W13_SLOTS,)), dma((2,)),
                dma(()), dma((nk, 2, nz // 2)), dma((nk,)),
                dma(()), dma((2, nz // 2)), dma(()),
                dma(()), dma((nj, 2, nz // 2)), dma((2,)), dma((nj,)),
            ],
            compiler_params=pltpu.CompilerParams(collective_id=0, has_side_effects=True, vmem_limit_bytes=67043328),
        )(x, meta, w1, w3, w2)

    rows = P(('data', 'expert'))
    wspec = P('expert')
    return jax.shard_map(local, mesh=mesh, in_specs=(rows, rows, rows, rows, wspec, wspec, wspec), out_specs=rows, check_vma=False)
```

```python
import functools

import jax
import jax.numpy as jnp
from jax import lax
from jax.experimental import pallas as pl
from jax.experimental.pallas import tpu as pltpu
from jax.sharding import PartitionSpec as P

F32 = jnp.float32
BF16 = jnp.bfloat16
RS_LAGS = (3, 5, 8, 11)
NP = 2


def _split3(v):
    hi = v.astype(BF16)
    r = v - hi.astype(F32)
    mid = r.astype(BF16)
    lo = (r - mid.astype(F32)).astype(BF16)
    return hi, mid, lo


def _kernel(cfg, x_ref, meta_ref, w1_ref, w3_ref, w2_ref, y_ref, xg, mg, w13, w2b, xs, u, hc, hh, pc, ph, qq, st, part, d2d, ring,
            x_sem, m_sem, w13_sem, w2_sem, ag_send, ag_recv, agd_recv, mg_send, mg_recv, mgd_recv, rs_send, rs_recv, rd_send, rd_recv):
    n, t, el, ch, cap, nc, nj, d_model, ff = cfg
    nz = n // 2
    half = nz // 2
    near = nz - half + 1
    blk = d_model // NP
    rc = 2 * cap
    rh = 2 * ch
    tt = 2 * t
    fcut = ff - ff % 256
    split = 2 * ff - fcut

    me = lax.axis_index('expert')
    z = me // 2
    c = me % 2
    right = ((z + 1) % nz) * 2 + c
    left = ((z + nz - 1) % nz) * 2 + c
    partner = z * 2 + (1 - c)
    nxt = (right, left)
    hot = me == 0
    cold = jnp.logical_not(hot)

    def remote(src, dst, ssem, rsem, dev):
        return pltpu.make_async_remote_copy(src_ref=src, dst_ref=dst, send_sem=ssem, recv_sem=rsem, device_id={'expert': dev},
                                            device_id_type=pl.DeviceIdType.MESH)

    def place(s, d):
        return 0 if s == 0 else nz - 1 if s == half else 2 * s - 1 if d == 0 else 2 * s

    def base(l):
        return 0 if l == 0 else nz * rh + (l - 1) * nz * rc

    def hops(k, d):
        return half - k % 2 if d == 0 else half - 1 + k % 2

    def w13_copies(e, slot):
        dst = w13.at[slot]
        sem = w13_sem.at[slot]
        out = [pltpu.make_async_copy(w1_ref.at[e], dst.at[:, pl.ds(0, ff)], sem)]
        if fcut < ff:
            out.append(pltpu.make_async_copy(w3_ref.at[e, :, pl.ds(fcut, ff - fcut)], dst.at[:, pl.ds(ff, ff - fcut)], sem))
        out.append(pltpu.make_async_copy(w3_ref.at[e, :, pl.ds(0, fcut)], dst.at[:, pl.ds(split, fcut)], sem))
        return out

    def w2_copies(j, slot):
        cols = pl.ds(pl.multiple_of(j * nc, nc), nc)
        return [pltpu.make_async_copy(w2_ref.at[l, :, cols], w2b.at[slot, l], w2_sem.at[slot]) for l in range(el)]

    def begin(copies):
        for cp in copies:
            cp.start()

    def done(copies):
        for cp in copies:
            cp.wait()

    x_copies = [pltpu.make_async_copy(x_ref.at[:, pl.ds(p * blk, blk)], xg.at[0, p, c], x_sem.at[p]) for p in range(NP)]
    m_copy = pltpu.make_async_copy(meta_ref, mg.at[0, c], m_sem)
    m_copy.start()
    begin(x_copies)
    for i in range(el - 1):
        begin(w13_copies(i + 1, i))
    for j in range(2):
        begin(w2_copies(j, j))

    barrier = pltpu.get_barrier_semaphore()
    for dev in (right, left, partner):
        pl.semaphore_signal(barrier, inc=1, device_id={'expert': dev}, device_id_type=pl.DeviceIdType.MESH)
    pl.semaphore_wait(barrier, 3)

    def share(q, p):
        src = xg.at[q, p, c]
        remote(src, src, ag_send, agd_recv.at[q, p], partner).start()

    def travels(s, d, p):
        return s < half or p == d

    def send(s, p):
        for d in range(2):
            if s <= half and travels(s, d, p):
                remote(xg.at[place(s - 1, d), p, c], xg.at[place(s, d), p, c], ag_send, ag_recv.at[d, s - 1, p], nxt[d]).start()

    def take(s, p):
        for d in range(2):
            if travels(s, d, p):
                dst = xg.at[place(s, d), p, c]
                remote(dst, dst, ag_send, ag_recv.at[d, s - 1, p], nxt[d]).wait_recv()
                if s < half and travels(s + 1, d, p):
                    remote(dst, xg.at[place(s + 1, d), p, c], ag_send, ag_recv.at[d, s, p], nxt[d]).start()
                share(place(s, d), p)

    def meta_send(s):
        for d in range(2):
            if s < half or (s == half and d == 0):
                remote(mg.at[place(s - 1, d), c], mg.at[place(s, d), c], mg_send, mg_recv.at[d, s - 1], nxt[d]).start()

    def meta_take(s):
        for d in range(2):
            if s < half or d == 0:
                dst = mg.at[place(s, d), c]
                remote(dst, dst, mg_send, mg_recv.at[d, s - 1], nxt[d]).wait_recv()
        meta_send(s + 1)
        for d in range(2):
            if s < half or d == 0:
                dst = mg.at[place(s, d), c]
                remote(dst, dst, mg_send, mgd_recv, partner).start()

    m_copy.wait()
    meta_send(1)
    remote(mg.at[0, c], mg.at[0, c], mg_send, mgd_recv, partner).start()
    x_copies[0].wait()
    send(1, 0)
    x_copies[1].wait()
    share(0, 0)
    share(0, 1)
    hc[...] = jnp.zeros(hc.shape, BF16)
    meta_take(1)
    send(1, 1)
    meta_take(2)
    take(1, 0)
    meta_take(3)
    take(1, 1)
    meta_take(4)

    def build():
        remote(mg.at[:, 0], mg.at[:, 0], mg_send, mgd_recv, partner).wait_recv()
        lane1 = lax.broadcasted_iota(jnp.int32, (8, tt), 1)
        s_i = lax.broadcasted_iota(jnp.int32, (tt, tt), 0)
        t_i = lax.broadcasted_iota(jnp.int32, (tt, tt), 1)
        upper = jnp.where((s_i < t_i) & (s_i // t == t_i // t), 1.0, 0.0).astype(BF16)
        core = (lax.broadcasted_iota(jnp.int32, (1, tt), 1) // t).astype(F32)
        row_c = lax.broadcasted_iota(jnp.int32, (el * rc, tt), 0).astype(F32)
        row_h = lax.broadcasted_iota(jnp.int32, (rh, tt), 0).astype(F32)
        col_c = lax.broadcasted_iota(jnp.int32, (tt, el * rc), 1).astype(F32)
        col_h = lax.broadcasted_iota(jnp.int32, (tt, rh), 1).astype(F32)
        far = jnp.full((1, tt), -4096.0, F32)

        def stats(q, carry):
            a = mg[q, 0]
            b = mg[q, 1]
            ids = jnp.where(lane1 < t, a, pltpu.roll(b, t, 1))
            gs = jnp.where(lane1 < t, pltpu.roll(a, t, 1), b)
            hits = [ids == (me * el + l).astype(F32) for l in range(el)]
            masks = [jnp.max(jnp.where(hit, 1.0, 0.0), axis=0, keepdims=True) for hit in hits]
            gates = [jnp.sum(jnp.where(hit, gs, 0.0), axis=0, keepdims=True) for hit in hits]
            st[0, q] = jnp.concatenate(masks + gates, axis=0)
            return carry

        lax.fori_loop(0, nz, stats, 0)
        every = st[0].reshape(nz * 2 * el, tt)
        st[1] = jnp.dot(every.astype(BF16), upper, preferred_element_type=F32).reshape(nz, 2 * el, tt)

        def fill(q, carry):
            mask = st[0, q]
            rank = st[1, q]
            codes = [jnp.where(mask[l:l + 1] > 0.0, core * cap + rank[l:l + 1] + float(l * rc), far) for l in range(el)]
            code_h = jnp.where(hot & (mask[0:1] > 0.0), core * ch + rank[0:1], far)
            codes[0] = jnp.where(hot, far, codes[0])
            rows = jnp.where(row_c == codes[0], 1.0, 0.0)
            for l in range(1, el):
                rows = jnp.where(row_c == codes[l], 1.0, rows)
            pc[q] = rows.astype(BF16)
            ph[q] = jnp.where(row_h == code_h, 1.0, 0.0).astype(BF16)
            cols = jnp.concatenate(codes + [mask[el:2 * el], code_h, jnp.zeros((128 - 2 * el - 1, tt), F32)], axis=0).T
            g = jnp.where(col_c == cols[:, 0:1], cols[:, el:el + 1], 0.0)
            for l in range(1, el):
                g = jnp.where(col_c == cols[:, l:l + 1], cols[:, el + l:el + l + 1], g)
            for p, piece in enumerate(_split3(g)):
                qq[q, :, p * el * rc:(p + 1) * el * rc] = piece
            g = jnp.where(col_h == cols[:, 2 * el:2 * el + 1], cols[:, el:el + 1], 0.0)
            qq[q, :, 3 * el * rc:] = jnp.concatenate(list(_split3(g)), axis=1)
            return carry

        lax.fori_loop(0, nz, fill, 0)

    build()
    take(2, 0)
    take(2, 1)

    def dispatch(first, count, is_hot):
        start = count * rh
        for i in range(count):
            q = first + i
            for p in range(NP):
                cols = slice(p * blk, (p + 1) * blk)
                xt = xg[q, p].reshape(tt, blk)
                res = jnp.dot(pc[q], xt, preferred_element_type=F32).astype(BF16)
                for l in range(1 if is_hot else 0, el):
                    row = (0 if l == 0 else start + (l - 1) * count * rc) + i * rc
                    xs[row:row + rc, cols] = res[l * rc:(l + 1) * rc]
                if is_hot:
                    xs[i * rh:(i + 1) * rh, cols] = jnp.dot(ph[q], xt, preferred_element_type=F32).astype(BF16)

    def products(xrow, urow, rows, slot):
        view = xs.at[pl.ds(xrow, rows)]
        out = pl.ds(urow, rows)

        def put(a, b, at):
            u[out, at] = (jax.nn.silu(a) * b).astype(BF16)

        for f in range(0, fcut, 256):
            put(jnp.dot(view[...], w13[slot, :, f:f + 256], preferred_element_type=F32),
                jnp.dot(view[...], w13[slot, :, split + f:split + f + 256], preferred_element_type=F32), slice(f, f + 256))
        if fcut < ff:
            ab = jnp.dot(view[...], w13[slot, :, fcut:split], preferred_element_type=F32)
            put(ab[:, :ff - fcut], ab[:, ff - fcut:], slice(fcut, ff))

    def one_pass(e, slot, first, count):
        @pl.when(hot & (e == 0))
        def _():
            products(0, first * rh, count * rh, slot)

        @pl.when(cold | (e > 0))
        def _():
            xrow = jnp.where(e == 0, 0, count * rh + (e - 1) * (count * rc))
            urow = jnp.where(e == 0, 0, nz * rh + (e - 1) * (nz * rc)) + first * rc
            products(pl.multiple_of(xrow, rc), pl.multiple_of(urow, rc), count * rc, slot)

    def gather_rows(first, count):
        for q in range(first, first + count):
            for p in range(NP):
                src = xg.at[q, p, 1 - c]
                remote(src, src, ag_send, agd_recv.at[q, p], partner).wait_recv()
        for is_hot, which in ((True, hot), (False, cold)):
            @pl.when(which)
            def _():
                dispatch(first, count, is_hot)

    gather_rows(0, near)

    def near_pass(i, carry):
        e = (i + 1) % el
        slot = i % (el - 1)
        done(w13_copies(e, slot))
        one_pass(e, slot, 0, near)

        @pl.when(i == 0)
        def _():
            begin(w13_copies(0, 0))
            take(3, 0)

        @pl.when(i == 1)
        def _():
            take(3, 1)

        return carry

    lax.fori_loop(0, el, near_pass, 0)
    take(4, 0)
    take(4, 1)
    gather_rows(near, nz - near)

    def far_pass(i, carry):
        e = (el - i) % el
        slot = (el - 1 - i) % (el - 1)

        @pl.when(i == el - 1)
        def _():
            done(w13_copies(1, 0))

        one_pass(e, slot, near, nz - near)

        @pl.when(i == 0)
        def _():
            begin(w13_copies(1, 0))

        return carry

    lax.fori_loop(0, el, far_pass, 0)

    def n_compute(j, slot, buf, is_hot):
        for l in range(el):
            big = is_hot and l == 0
            step = rh if big else rc
            h = jnp.dot(u[base(l):base(l) + nz * step, :], w2b[slot, l], preferred_element_type=F32).astype(BF16)
            for q in range(nz):
                if big:
                    hh[q] = h[q * rh:(q + 1) * rh]
                else:
                    hc[q, l * rc:(l + 1) * rc, :] = h[q * rc:(q + 1) * rc]
        for q in range(nz):
            if is_hot:
                tot = jnp.dot(qq[q], jnp.concatenate([hc[q]] * 3 + [hh[q]] * 3, axis=0), preferred_element_type=F32)
            else:
                tot = jnp.dot(qq[q, :, :3 * el * rc], jnp.concatenate([hc[q]] * 3, axis=0), preferred_element_type=F32)
            part[buf, q] = tot.reshape(2, t, nc)

    def d2d_copy(j, buf):
        return remote(part.at[buf, :, 1 - c], d2d.at[j], rd_send.at[buf], rd_recv.at[j], partner)

    def slot_of(s, d):
        return s - 1 if d == 0 else nz - 1 - s

    def rs_start(j):
        buf = j % 2
        d2d_copy(j, buf).wait_recv()
        for d in range(nz):
            d2d[j, d] += part[buf, d, c]
        for d in range(2):
            h = hops(j, d)
            dest = h + half - 1 if d == 0 else 2 * h - 1
            remote(d2d.at[j, dest], ring.at[j, slot_of(1, d)], rs_send, rs_recv.at[j, d, 0], nxt[d]).start()

    def rs_event(j, s, d):
        h = hops(j, d)
        dest = 2 * (h - s) if d == 0 else 2 * (h - s) - 1
        at = slot_of(s, d)
        here = ring.at[j, at]
        remote(here, here, rs_send, rs_recv.at[j, d, s - 1], nxt[d]).wait_recv()

        @pl.when(s < h)
        def _():
            ring[j, at] += d2d[j, dest]
            remote(here, ring.at[j, slot_of(s % half + 1, d)], rs_send, rs_recv.at[j, d, s % half], nxt[d]).start()

        @pl.when(s == h)
        def _():
            d2d[j, 0] += ring[j, at]

    def rs_round(r, carry):
        @pl.when(r < nj)
        def _():
            slot = r % 2
            for cp in w2_copies(r, slot):
                cp.wait()

            @pl.when(r >= 2)
            def _():
                d2d_copy(r - 2, slot).wait_send()

            @pl.when(hot)
            def _():
                n_compute(r, slot, slot, True)

            @pl.when(jnp.logical_not(hot))
            def _():
                n_compute(r, slot, slot, False)

            d2d_copy(r, slot).start()

            @pl.when(r + 2 < nj)
            def _():
                for cp in w2_copies(r + 2, slot):
                    cp.start()

        @pl.when((r >= 1) & (r - 1 < nj))
        def _():
            rs_start(r - 1)

        for s in range(1, half + 1):
            j = r - RS_LAGS[s - 1]
            for d in range(2):
                @pl.when((j >= 0) & (j < nj) & (s <= hops(j, d)))
                def _():
                    rs_event(j, s, d)

        j = r - RS_LAGS[half - 1]

        @pl.when((j >= 0) & (j < nj))
        def _():
            y_ref[:, pl.ds(pl.multiple_of(j * nc, nc), nc)] = d2d[j, 0].astype(BF16)

        return carry

    lax.fori_loop(0, nj + RS_LAGS[half - 1], rs_round, 0)

    for j in range(max(nj - 2, 0), nj):
        d2d_copy(j, j % 2).wait_send()
    for buf, sem in ((mg, mg_send), (xg, ag_send)):
        for view in (buf.at[pl.ds(0, nz - 1)], buf.at[nz - 1, 0]):
            remote(view, view, sem, mgd_recv, partner).wait_send()
    for j in range(nj):
        blk = ring.at[j]
        remote(blk, blk, rs_send, rs_recv.at[j, 0, 0], partner).wait_send()


def solution(mesh):
    n = mesh.shape['expert']

    def local(x, idx, g, hot_tok, w1, w3, w2):
        t, d = x.shape
        k = idx.shape[1]
        el, _, ff = w1.shape
        e = el * n
        ch = hot_tok.shape[0]
        need = 2 * ((t * k - ch + e - 2) // (e - 1))
        cap = -(-need // 16) * 16
        nc = 256
        nj = d // nc
        nz = n // 2
        near = nz - nz // 2 + 1
        rows = nz * 2 * (ch + (el - 1) * cap)
        xrows = near * 2 * (ch + (el - 1) * cap)
        ids = jnp.pad(idx.T.astype(F32), ((0, 8 - k), (0, 0)), constant_values=-1.0)
        meta = jnp.concatenate([ids, jnp.pad(g.T, ((0, 8 - k), (0, 0)))], axis=1)
        cfg = (n, t, el, ch, cap, nc, nj, d, ff)
        dma = pltpu.SemaphoreType.DMA
        return pl.pallas_call(
            functools.partial(_kernel, cfg),
            name='moe',
            out_shape=jax.ShapeDtypeStruct((t, d), BF16),
            in_specs=[pl.BlockSpec(memory_space=pl.ANY)] * 5,
            out_specs=pl.BlockSpec(memory_space=pltpu.VMEM),
            scratch_shapes=[
                pltpu.VMEM((nz, NP, 2, t, d // NP), BF16),
                pltpu.VMEM((nz, 2, 8, 2 * t), F32),
                pltpu.VMEM((el - 1, d, 2 * ff), BF16),
                pltpu.VMEM((2, el, ff, nc), BF16),
                pltpu.VMEM((xrows, d), BF16),
                pltpu.VMEM((rows, ff), BF16),
                pltpu.VMEM((nz, el * 2 * cap, nc), BF16),
                pltpu.VMEM((nz, 2 * ch, nc), BF16),
                pltpu.VMEM((nz, el * 2 * cap, 2 * t), BF16),
                pltpu.VMEM((nz, 2 * ch, 2 * t), BF16),
                pltpu.VMEM((nz, 2 * t, 6 * (el * cap + ch)), BF16),
                pltpu.VMEM((2, nz, 2 * el, 2 * t), F32),
                pltpu.VMEM((2, nz, 2, t, nc), F32),
                pltpu.VMEM((nj, nz, t, nc), F32),
                pltpu.VMEM((nj, nz - 1, t, nc), F32),
                dma((NP,)), dma(()), dma((el - 1,)), dma((2,)),
                dma(()), dma((2, nz // 2, NP)), dma((nz, NP)),
                dma(()), dma((2, nz // 2)), dma(()),
                dma(()), dma((nj, 2, nz // 2)), dma((2,)), dma((nj,)),
            ],
            compiler_params=pltpu.CompilerParams(collective_id=0, has_side_effects=True, vmem_limit_bytes=67043328),
        )(x, meta, w1, w3, w2)

    rows = P(('data', 'expert'))
    wspec = P('expert')
    return jax.shard_map(local, mesh=mesh, in_specs=(rows, rows, rows, rows, wspec, wspec, wspec), out_specs=rows, check_vma=False)
```

```python
import functools

import jax
import jax.numpy as jnp
from jax import lax
from jax.experimental import pallas as pl
from jax.experimental.pallas import tpu as pltpu
from jax.sharding import PartitionSpec as P

F32 = jnp.float32
BF16 = jnp.bfloat16
RS_LAGS = (3, 5, 8, 11)
NP = 2


def _split3(v):
    hi = v.astype(BF16)
    r = v - hi.astype(F32)
    mid = r.astype(BF16)
    lo = (r - mid.astype(F32)).astype(BF16)
    return hi, mid, lo


def _kernel(cfg, x_ref, meta_ref, w1_ref, w3_ref, w2_ref, y_ref, xg, mg, w13, w2b, xs, u, hc, hh, pc, ph, qq, st, part, d2d, ring,
            x_sem, m_sem, w13_sem, w2_sem, ag_send, ag_recv, agd_recv, mg_send, mg_recv, mgd_recv, rs_send, rs_recv, rd_send, rd_recv):
    n, t, el, ch, cap, nc, nj, d_model, ff = cfg
    nz = n // 2
    half = nz // 2
    near = nz - half + 1
    blk = d_model // NP
    rc = 2 * cap
    rh = 2 * ch
    tt = 2 * t
    fcut = ff - ff % 256
    split = 2 * ff - fcut

    me = lax.axis_index('expert')
    z = me // 2
    c = me % 2
    right = ((z + 1) % nz) * 2 + c
    left = ((z + nz - 1) % nz) * 2 + c
    partner = z * 2 + (1 - c)
    nxt = (right, left)
    hot = me == 0
    cold = jnp.logical_not(hot)

    def remote(src, dst, ssem, rsem, dev):
        return pltpu.make_async_remote_copy(src_ref=src, dst_ref=dst, send_sem=ssem, recv_sem=rsem, device_id={'expert': dev},
                                            device_id_type=pl.DeviceIdType.MESH)

    def place(s, d):
        return 0 if s == 0 else nz - 1 if s == half else 2 * s - 1 if d == 0 else 2 * s

    def base(l):
        return 0 if l == 0 else nz * rh + (l - 1) * nz * rc

    def hops(k, d):
        return half - k % 2 if d == 0 else half - 1 + k % 2

    def w13_copies(e, slot):
        dst = w13.at[slot]
        sem = w13_sem.at[slot]
        out = [pltpu.make_async_copy(w1_ref.at[e], dst.at[:, pl.ds(0, ff)], sem)]
        if fcut < ff:
            out.append(pltpu.make_async_copy(w3_ref.at[e, :, pl.ds(fcut, ff - fcut)], dst.at[:, pl.ds(ff, ff - fcut)], sem))
        out.append(pltpu.make_async_copy(w3_ref.at[e, :, pl.ds(0, fcut)], dst.at[:, pl.ds(split, fcut)], sem))
        return out

    def w2_copies(j, slot):
        cols = pl.ds(pl.multiple_of(j * nc, nc), nc)
        return [pltpu.make_async_copy(w2_ref.at[l, :, cols], w2b.at[slot, l], w2_sem.at[slot]) for l in range(el)]

    def begin(copies):
        for cp in copies:
            cp.start()

    def done(copies):
        for cp in copies:
            cp.wait()

    x_copies = [pltpu.make_async_copy(x_ref.at[:, pl.ds(p * blk, blk)], xg.at[0, p, c], x_sem.at[p]) for p in range(NP)]
    m_copy = pltpu.make_async_copy(meta_ref, mg.at[0, c], m_sem)
    m_copy.start()
    for cp in x_copies:
        cp.start()

    barrier = pltpu.get_barrier_semaphore()
    for dev in (right, left, partner):
        pl.semaphore_signal(barrier, inc=1, device_id={'expert': dev}, device_id_type=pl.DeviceIdType.MESH)
    pl.semaphore_wait(barrier, 3)

    def share(q, p):
        src = xg.at[q, p, c]
        remote(src, src, ag_send, agd_recv.at[q, p], partner).start()

    def travels(s, d, p):
        return s < half or p == d

    def send(s, p):
        for d in range(2):
            if s <= half and travels(s, d, p):
                remote(xg.at[place(s - 1, d), p, c], xg.at[place(s, d), p, c], ag_send, ag_recv.at[d, s - 1, p], nxt[d]).start()

    def take(s, p):
        for d in range(2):
            if travels(s, d, p):
                dst = xg.at[place(s, d), p, c]
                remote(dst, dst, ag_send, ag_recv.at[d, s - 1, p], nxt[d]).wait_recv()
                if s < half and travels(s + 1, d, p):
                    remote(dst, xg.at[place(s + 1, d), p, c], ag_send, ag_recv.at[d, s, p], nxt[d]).start()
                share(place(s, d), p)

    def meta_send(s):
        for d in range(2):
            if s < half or (s == half and d == 0):
                remote(mg.at[place(s - 1, d), c], mg.at[place(s, d), c], mg_send, mg_recv.at[d, s - 1], nxt[d]).start()

    def meta_take(s):
        for d in range(2):
            if s < half or d == 0:
                dst = mg.at[place(s, d), c]
                remote(dst, dst, mg_send, mg_recv.at[d, s - 1], nxt[d]).wait_recv()
        meta_send(s + 1)
        for d in range(2):
            if s < half or d == 0:
                dst = mg.at[place(s, d), c]
                remote(dst, dst, mg_send, mgd_recv, partner).start()

    m_copy.wait()
    meta_send(1)
    remote(mg.at[0, c], mg.at[0, c], mg_send, mgd_recv, partner).start()
    x_copies[0].wait()
    send(1, 0)
    begin(w13_copies(1, 0))
    meta_take(1)
    x_copies[1].wait()
    send(1, 1)
    share(0, 0)
    share(0, 1)
    hc[...] = jnp.zeros(hc.shape, BF16)
    meta_take(2)
    take(1, 0)
    begin(w13_copies(2, 1))
    meta_take(3)
    take(1, 1)
    begin(w13_copies(3, 2))
    meta_take(4)

    def build():
        remote(mg.at[:, 0], mg.at[:, 0], mg_send, mgd_recv, partner).wait_recv()
        lane1 = lax.broadcasted_iota(jnp.int32, (8, tt), 1)
        s_i = lax.broadcasted_iota(jnp.int32, (tt, tt), 0)
        t_i = lax.broadcasted_iota(jnp.int32, (tt, tt), 1)
        upper = jnp.where((s_i < t_i) & (s_i // t == t_i // t), 1.0, 0.0).astype(BF16)
        core = (lax.broadcasted_iota(jnp.int32, (1, tt), 1) // t).astype(F32)
        row_c = lax.broadcasted_iota(jnp.int32, (el * rc, tt), 0).astype(F32)
        row_h = lax.broadcasted_iota(jnp.int32, (rh, tt), 0).astype(F32)
        col_c = lax.broadcasted_iota(jnp.int32, (tt, el * rc), 1).astype(F32)
        col_h = lax.broadcasted_iota(jnp.int32, (tt, rh), 1).astype(F32)
        far = jnp.full((1, tt), -4096.0, F32)

        def stats(q, carry):
            a = mg[q, 0]
            b = mg[q, 1]
            ids = jnp.where(lane1 < t, a, pltpu.roll(b, t, 1))
            gs = jnp.where(lane1 < t, pltpu.roll(a, t, 1), b)
            hits = [ids == (me * el + l).astype(F32) for l in range(el)]
            masks = [jnp.max(jnp.where(hit, 1.0, 0.0), axis=0, keepdims=True) for hit in hits]
            gates = [jnp.sum(jnp.where(hit, gs, 0.0), axis=0, keepdims=True) for hit in hits]
            st[0, q] = jnp.concatenate(masks + gates, axis=0)
            return carry

        lax.fori_loop(0, nz, stats, 0)
        every = st[0].reshape(nz * 2 * el, tt)
        st[1] = jnp.dot(every.astype(BF16), upper, preferred_element_type=F32).reshape(nz, 2 * el, tt)

        def fill(q, carry):
            mask = st[0, q]
            rank = st[1, q]
            codes = [jnp.where(mask[l:l + 1] > 0.0, core * cap + rank[l:l + 1] + float(l * rc), far) for l in range(el)]
            code_h = jnp.where(hot & (mask[0:1] > 0.0), core * ch + rank[0:1], far)
            codes[0] = jnp.where(hot, far, codes[0])
            rows = jnp.where(row_c == codes[0], 1.0, 0.0)
            for l in range(1, el):
                rows = jnp.where(row_c == codes[l], 1.0, rows)
            pc[q] = rows.astype(BF16)
            ph[q] = jnp.where(row_h == code_h, 1.0, 0.0).astype(BF16)
            cols = jnp.concatenate(codes + [mask[el:2 * el], code_h, jnp.zeros((128 - 2 * el - 1, tt), F32)], axis=0).T
            g = jnp.where(col_c == cols[:, 0:1], cols[:, el:el + 1], 0.0)
            for l in range(1, el):
                g = jnp.where(col_c == cols[:, l:l + 1], cols[:, el + l:el + l + 1], g)
            for p, piece in enumerate(_split3(g)):
                qq[q, :, p * el * rc:(p + 1) * el * rc] = piece
            g = jnp.where(col_h == cols[:, 2 * el:2 * el + 1], cols[:, el:el + 1], 0.0)
            qq[q, :, 3 * el * rc:] = jnp.concatenate(list(_split3(g)), axis=1)
            return carry

        lax.fori_loop(0, nz, fill, 0)

    build()
    take(2, 0)
    take(2, 1)
    for j in range(2):
        begin(w2_copies(j, j))

    def dispatch(first, count, is_hot):
        start = count * rh
        for i in range(count):
            q = first + i
            for p in range(NP):
                cols = slice(p * blk, (p + 1) * blk)
                xt = xg[q, p].reshape(tt, blk)
                res = jnp.dot(pc[q], xt, preferred_element_type=F32).astype(BF16)
                for l in range(1 if is_hot else 0, el):
                    row = (0 if l == 0 else start + (l - 1) * count * rc) + i * rc
                    xs[row:row + rc, cols] = res[l * rc:(l + 1) * rc]
                if is_hot:
                    xs[i * rh:(i + 1) * rh, cols] = jnp.dot(ph[q], xt, preferred_element_type=F32).astype(BF16)

    def products(xrow, urow, rows, slot):
        view = xs.at[pl.ds(xrow, rows)]
        out = pl.ds(urow, rows)

        def put(a, b, at):
            u[out, at] = (jax.nn.silu(a) * b).astype(BF16)

        for f in range(0, fcut, 256):
            put(jnp.dot(view[...], w13[slot, :, f:f + 256], preferred_element_type=F32),
                jnp.dot(view[...], w13[slot, :, split + f:split + f + 256], preferred_element_type=F32), slice(f, f + 256))
        if fcut < ff:
            ab = jnp.dot(view[...], w13[slot, :, fcut:split], preferred_element_type=F32)
            put(ab[:, :ff - fcut], ab[:, ff - fcut:], slice(fcut, ff))

    def one_pass(e, slot, first, count):
        @pl.when(hot & (e == 0))
        def _():
            products(0, first * rh, count * rh, slot)

        @pl.when(cold | (e > 0))
        def _():
            xrow = jnp.where(e == 0, 0, count * rh + (e - 1) * (count * rc))
            urow = jnp.where(e == 0, 0, nz * rh + (e - 1) * (nz * rc)) + first * rc
            products(pl.multiple_of(xrow, rc), pl.multiple_of(urow, rc), count * rc, slot)

    def gather_rows(first, count):
        for q in range(first, first + count):
            for p in range(NP):
                src = xg.at[q, p, 1 - c]
                remote(src, src, ag_send, agd_recv.at[q, p], partner).wait_recv()
        for is_hot, which in ((True, hot), (False, cold)):
            @pl.when(which)
            def _():
                dispatch(first, count, is_hot)

    gather_rows(0, near)

    def near_pass(i, carry):
        e = (i + 1) % el
        slot = i % (el - 1)
        done(w13_copies(e, slot))
        one_pass(e, slot, 0, near)

        @pl.when(i == 0)
        def _():
            begin(w13_copies(0, 0))
            take(3, 0)

        @pl.when(i == 1)
        def _():
            take(3, 1)

        return carry

    lax.fori_loop(0, el, near_pass, 0)
    take(4, 0)
    take(4, 1)
    gather_rows(near, nz - near)

    def far_pass(i, carry):
        e = (el - i) % el
        slot = (el - 1 - i) % (el - 1)

        @pl.when(i == el - 1)
        def _():
            done(w13_copies(1, 0))

        one_pass(e, slot, near, nz - near)

        @pl.when(i == 0)
        def _():
            begin(w13_copies(1, 0))

        return carry

    lax.fori_loop(0, el, far_pass, 0)

    def n_compute(j, slot, buf, is_hot):
        for l in range(el):
            big = is_hot and l == 0
            step = rh if big else rc
            h = jnp.dot(u[base(l):base(l) + nz * step, :], w2b[slot, l], preferred_element_type=F32).astype(BF16)
            for q in range(nz):
                if big:
                    hh[q] = h[q * rh:(q + 1) * rh]
                else:
                    hc[q, l * rc:(l + 1) * rc, :] = h[q * rc:(q + 1) * rc]
        for q in range(nz):
            if is_hot:
                tot = jnp.dot(qq[q], jnp.concatenate([hc[q]] * 3 + [hh[q]] * 3, axis=0), preferred_element_type=F32)
            else:
                tot = jnp.dot(qq[q, :, :3 * el * rc], jnp.concatenate([hc[q]] * 3, axis=0), preferred_element_type=F32)
            part[buf, q] = tot.reshape(2, t, nc)

    def d2d_copy(j, buf):
        return remote(part.at[buf, :, 1 - c], d2d.at[j], rd_send.at[buf], rd_recv.at[j], partner)

    def slot_of(s, d):
        return s - 1 if d == 0 else nz - 1 - s

    def rs_start(j):
        buf = j % 2
        d2d_copy(j, buf).wait_recv()
        for d in range(nz):
            d2d[j, d] += part[buf, d, c]
        for d in range(2):
            h = hops(j, d)
            dest = h + half - 1 if d == 0 else 2 * h - 1
            remote(d2d.at[j, dest], ring.at[j, slot_of(1, d)], rs_send, rs_recv.at[j, d, 0], nxt[d]).start()

    def rs_event(j, s, d):
        h = hops(j, d)
        dest = 2 * (h - s) if d == 0 else 2 * (h - s) - 1
        at = slot_of(s, d)
        here = ring.at[j, at]
        remote(here, here, rs_send, rs_recv.at[j, d, s - 1], nxt[d]).wait_recv()

        @pl.when(s < h)
        def _():
            ring[j, at] += d2d[j, dest]
            remote(here, ring.at[j, slot_of(s % half + 1, d)], rs_send, rs_recv.at[j, d, s % half], nxt[d]).start()

        @pl.when(s == h)
        def _():
            d2d[j, 0] += ring[j, at]

    def rs_round(r, carry):
        @pl.when(r < nj)
        def _():
            slot = r % 2
            for cp in w2_copies(r, slot):
                cp.wait()

            @pl.when(r >= 2)
            def _():
                d2d_copy(r - 2, slot).wait_send()

            @pl.when(hot)
            def _():
                n_compute(r, slot, slot, True)

            @pl.when(jnp.logical_not(hot))
            def _():
                n_compute(r, slot, slot, False)

            d2d_copy(r, slot).start()

            @pl.when(r + 2 < nj)
            def _():
                for cp in w2_copies(r + 2, slot):
                    cp.start()

        @pl.when((r >= 1) & (r - 1 < nj))
        def _():
            rs_start(r - 1)

        for s in range(1, half + 1):
            j = r - RS_LAGS[s - 1]
            for d in range(2):
                @pl.when((j >= 0) & (j < nj) & (s <= hops(j, d)))
                def _():
                    rs_event(j, s, d)

        j = r - RS_LAGS[half - 1]

        @pl.when((j >= 0) & (j < nj))
        def _():
            y_ref[:, pl.ds(pl.multiple_of(j * nc, nc), nc)] = d2d[j, 0].astype(BF16)

        return carry

    lax.fori_loop(0, nj + RS_LAGS[half - 1], rs_round, 0)

    for j in range(max(nj - 2, 0), nj):
        d2d_copy(j, j % 2).wait_send()
    for buf, sem in ((mg, mg_send), (xg, ag_send)):
        for view in (buf.at[pl.ds(0, nz - 1)], buf.at[nz - 1, 0]):
            remote(view, view, sem, mgd_recv, partner).wait_send()
    for j in range(nj):
        blk = ring.at[j]
        remote(blk, blk, rs_send, rs_recv.at[j, 0, 0], partner).wait_send()


def solution(mesh):
    n = mesh.shape['expert']

    def local(x, idx, g, hot_tok, w1, w3, w2):
        t, d = x.shape
        k = idx.shape[1]
        el, _, ff = w1.shape
        e = el * n
        ch = hot_tok.shape[0]
        need = 2 * ((t * k - ch + e - 2) // (e - 1))
        cap = -(-need // 16) * 16
        nc = 256
        nj = d // nc
        nz = n // 2
        near = nz - nz // 2 + 1
        rows = nz * 2 * (ch + (el - 1) * cap)
        xrows = near * 2 * (ch + (el - 1) * cap)
        ids = jnp.pad(idx.T.astype(F32), ((0, 8 - k), (0, 0)), constant_values=-1.0)
        meta = jnp.concatenate([ids, jnp.pad(g.T, ((0, 8 - k), (0, 0)))], axis=1)
        cfg = (n, t, el, ch, cap, nc, nj, d, ff)
        dma = pltpu.SemaphoreType.DMA
        return pl.pallas_call(
            functools.partial(_kernel, cfg),
            name='moe',
            out_shape=jax.ShapeDtypeStruct((t, d), BF16),
            in_specs=[pl.BlockSpec(memory_space=pl.ANY)] * 5,
            out_specs=pl.BlockSpec(memory_space=pltpu.VMEM),
            scratch_shapes=[
                pltpu.VMEM((nz, NP, 2, t, d // NP), BF16),
                pltpu.VMEM((nz, 2, 8, 2 * t), F32),
                pltpu.VMEM((el - 1, d, 2 * ff), BF16),
                pltpu.VMEM((2, el, ff, nc), BF16),
                pltpu.VMEM((xrows, d), BF16),
                pltpu.VMEM((rows, ff), BF16),
                pltpu.VMEM((nz, el * 2 * cap, nc), BF16),
                pltpu.VMEM((nz, 2 * ch, nc), BF16),
                pltpu.VMEM((nz, el * 2 * cap, 2 * t), BF16),
                pltpu.VMEM((nz, 2 * ch, 2 * t), BF16),
                pltpu.VMEM((nz, 2 * t, 6 * (el * cap + ch)), BF16),
                pltpu.VMEM((2, nz, 2 * el, 2 * t), F32),
                pltpu.VMEM((2, nz, 2, t, nc), F32),
                pltpu.VMEM((nj, nz, t, nc), F32),
                pltpu.VMEM((nj, nz - 1, t, nc), F32),
                dma((NP,)), dma(()), dma((el - 1,)), dma((2,)),
                dma(()), dma((2, nz // 2, NP)), dma((nz, NP)),
                dma(()), dma((2, nz // 2)), dma(()),
                dma(()), dma((nj, 2, nz // 2)), dma((2,)), dma((nj,)),
            ],
            compiler_params=pltpu.CompilerParams(collective_id=0, has_side_effects=True, vmem_limit_bytes=67043328),
        )(x, meta, w1, w3, w2)

    rows = P(('data', 'expert'))
    wspec = P('expert')
    return jax.shard_map(local, mesh=mesh, in_specs=(rows, rows, rows, rows, wspec, wspec, wspec), out_specs=rows, check_vma=False)
```
